32 devices in a mesh: groups: 2 (over y), shell: 8 (over z, x), batch: 2 (over core).
Axes of the slice: x: 2, y: 2, z: 4, core: 2. Of those that a mesh axis runs over, the one named last changes fastest.
Arguments:
- particles: bfloat16 [320, 1024], P(('groups', 'batch'), 'shell'), parts along dimension 0, may hold values from -5 to 5
- classes: bfloat16 [512, 1024], P('groups', 'shell'), parts along dimension 0, may hold values from -2.5 to 2.5
- ctf: float32 [16, 512], P('groups', 'shell'), parts along dimension 0, may hold values from 0.1 to 1
- sigma2: float32 [128], P('groups'), parts along dimension 0, may hold values from 0.5 to 8
- shell_of: int32 [512], P('shell'), may hold values from 0 to 63, as said below
- rot_table: int32 [48, 512], P(None, 'shell'), may hold values from 0 to 511, as said below
- ctf_group: int32 [320], P(('groups', 'batch')), parts along dimension 0, may hold values from 0 to 7
Outputs:
- class_sums: float32 [512, 1024], P('groups', 'shell'), parts along dimension 0
- class_weights: float32 [512, 512], P('groups', 'shell'), parts along dimension 0
- log_evidence: float32 [320], P(('groups', 'batch')), parts along dimension 0
The draws below stay inside these ranges and needn't reach their ends.
There are 2 independent parts, one for each index of `groups`. The reference program is written for one: setup_inputs(seed, part) draws one part's arguments, and reference() takes and returns one part's arrays. A program takes and returns all parts, laid end to end along the dimension named above; an argument that names none is the same for every part. Nothing has to cross between parts.
Inputs may be any that keep to these rules, and one draw needn't show every extreme that they name: shell_of never falls along the coefficients; its first entry is 0 and its last 63. `rot_table`: for each rotation, each aligned block of 64 coefficients is mapped onto itself one to one; rotation 0 maps every coefficient to itself.
All inputs are finite; a program needn't handle non-finite values.
Results may differ from the reference program's by a relative error of at most 0.0041.
Values may be sent and summed in bfloat16 or wider, within the bound.
No kernel may reach another device: no remote copies, remote signals or barrier semaphores. Data moves between devices by JAX's collectives and lax.ppermute only.
A program may use at most 64 MiB of HBM per device.

```python
import math
import jax
import jax.numpy as jnp
from jax import lax

K = 256
ROT = 48
CO_DEV = 64
SHELLS = 64
CTFG = 8
COEF = 512
PARTICLES = 160
N_SHELL = 8


def particle_field(key):
    shape = (PARTICLES, 2 * COEF)
    return jnp.clip(jax.random.normal(jax.random.fold_in(key, 11), shape, jnp.float32), -5.0, 5.0)


def draw_particles(key, part):
    return particle_field(key).astype(jnp.bfloat16)


def draw_classes(key, part):
    noise = jnp.clip(jax.random.normal(jax.random.fold_in(key, 21), (K, 2 * COEF), jnp.float32), -5.0, 5.0) * 0.02
    return noise.astype(jnp.bfloat16)


def draw_shell_of(key, part):
    values = jnp.sort(jax.random.randint(key, (COEF,), 0, SHELLS, dtype=jnp.int32))
    values = values.at[0].set(0).at[COEF - 1].set(SHELLS - 1)
    return values.astype(jnp.int32)


def draw_rot_table(key, part):
    blocks = COEF // CO_DEV
    ranks = jnp.arange(CO_DEV, dtype=jnp.int32)
    keyed = jax.random.randint(key, (ROT, blocks, CO_DEV), 0, 1048576, dtype=jnp.int32) * CO_DEV + ranks
    order = jnp.argsort(keyed, axis=-1, stable=True).astype(jnp.int32)
    identity = jnp.broadcast_to(ranks, (blocks, CO_DEV))
    order = order.at[0].set(identity)
    offsets = (jnp.arange(blocks, dtype=jnp.int32) * CO_DEV)[None, :, None]
    return (order + offsets).reshape(ROT, COEF).astype(jnp.int32)


def touch_ends(values, stream_key, least, high):
    longest = values.shape.index(max(values.shape))
    spots = []
    for shift in (0, 1):
        where = [jax.random.randint(jax.random.fold_in(stream_key, axis), (), 0, length) for axis, length in enumerate(values.shape)]
        where[longest] = (where[longest] + shift) % values.shape[longest]
        spots.append(tuple(where))
    return values.at[spots[0]].set(least).at[spots[1]].set(high)


def levels(own_key, extent, split, low, high):
    factor_of, own = 1.0, jax.random.fold_in(own_key, 6)
    for dim, shards_of in split:
        draws = jnp.exp(jax.random.uniform(jax.random.fold_in(own, dim), (shards_of,), jnp.float32, low / len(split), high / len(split)))
        factor_of = factor_of * jnp.repeat(draws, extent[dim] // shards_of).reshape([-1 if axis == dim else 1 for axis in range(len(extent))])
    return factor_of


def setup_inputs(seed: int = 0, part: int = 0) -> dict:
    seeds = jax.random.split(jax.random.key(seed), 8)
    own_keys = jax.random.split(jax.random.fold_in(seeds[7], part), 8)
    return {
        "particles": draw_particles(jax.random.fold_in(jax.random.fold_in(seeds[7], part), 71), part),
        "classes": draw_classes(jax.random.fold_in(jax.random.fold_in(seeds[7], part), 71), part),
        "ctf": jnp.clip(0.1 + 0.9 * jax.random.uniform(own_keys[2], (CTFG, COEF), jnp.float32) ** levels(own_keys[2], (CTFG, COEF), ((1, 8),), -0.2, 0.2), 0.1, 1.0),
        "sigma2": jnp.clip(jnp.exp(jax.random.uniform(own_keys[3], (SHELLS,), jnp.float32, math.log(0.5), math.log(8.0))), 0.5, 8.0),
        "shell_of": draw_shell_of(jax.random.fold_in(seeds[7], 71), part),
        "rot_table": draw_rot_table(jax.random.fold_in(seeds[7], 71), part),
        "ctf_group": touch_ends(jax.random.randint(own_keys[6], (PARTICLES,), 0, CTFG), jax.random.fold_in(own_keys[6], 1), 0, CTFG - 1).astype(jnp.int32),
    }


def halves(array):
    rows = array.shape[0]
    blocks = array.reshape(rows, N_SHELL, 2, CO_DEV)
    return blocks[:, :, 0, :].reshape(rows, COEF), blocks[:, :, 1, :].reshape(rows, COEF)


def join_parts(real_part, imag_part):
    rows = real_part.shape[0]
    stacked = jnp.stack([real_part.reshape(rows, N_SHELL, CO_DEV), imag_part.reshape(rows, N_SHELL, CO_DEV)], axis=2)
    return stacked.reshape(rows, 2 * COEF)


def reference(particles, classes, ctf, sigma2, shell_of, rot_table, ctf_group):
    highest = lax.Precision.HIGHEST
    weight = 1.0 / sigma2[shell_of]
    real_part, imag_part = halves(particles.astype(jnp.float32))
    class_real, class_imag = halves(classes)
    ctf_part = ctf[ctf_group]
    weighted_ctf = weight[None, :] * ctf_part
    weighted_real = (weighted_ctf * real_part).astype(jnp.bfloat16)
    weighted_imag = (weighted_ctf * imag_part).astype(jnp.bfloat16)
    ctf_power = weight[None, :] * ctf * ctf

    def score_rotation(table_row):
        rot_real = class_real[:, table_row]
        rot_imag = class_imag[:, table_row]
        cross_terms = jnp.dot(weighted_real, rot_real.T, preferred_element_type=jnp.float32)
        cross_terms = cross_terms + jnp.dot(weighted_imag, rot_imag.T, preferred_element_type=jnp.float32)
        class_power = rot_real.astype(jnp.float32) ** 2 + rot_imag.astype(jnp.float32) ** 2
        penalty = jnp.dot(ctf_power, class_power.T, precision=highest, preferred_element_type=jnp.float32)
        return cross_terms - 0.5 * penalty[ctf_group]

    scores = lax.map(score_rotation, rot_table)
    scores = jnp.transpose(scores, (1, 2, 0)).reshape(PARTICLES, K * ROT)
    peak = jnp.max(scores, axis=1)
    log_evidence = peak + jnp.log(jnp.sum(jnp.exp(scores - peak[:, None]), axis=1))
    posterior = jnp.exp(scores - log_evidence[:, None]).astype(jnp.bfloat16).reshape(PARTICLES, K, ROT)
    sources = jnp.concatenate([ctf_part * real_part, ctf_part * imag_part, ctf_part * ctf_part], axis=1).astype(jnp.bfloat16)

    def add_rotation(totals, inputs):
        post_rot, table_row = inputs
        frame = jnp.dot(post_rot.T, sources, preferred_element_type=jnp.float32).reshape(K, 3, COEF)
        return totals.at[:, :, table_row].add(frame), None

    totals, unused = lax.scan(add_rotation, jnp.zeros((K, 3, COEF), jnp.float32), (jnp.transpose(posterior, (2, 0, 1)), rot_table))
    class_sums = join_parts(totals[:, 0], totals[:, 1])
    return class_sums, totals[:, 2], log_evidence
```

```python
import jax
import jax.numpy as jnp
from jax import lax
from jax.experimental import pallas as pl
from jax.experimental.pallas import tpu as pltpu
from jax.sharding import PartitionSpec as P

HIGHEST = lax.Precision.HIGHEST


def round_up(value, step):
    return -(-value // step) * step


def row_plan(class_count, particle_count, rotations, group_count):
    weighted_at = round_up(class_count, 16)
    inverse_at = weighted_at + round_up(particle_count, 16)
    power_at = inverse_at + round_up(rotations, 16)
    return weighted_at, inverse_at, power_at, power_at + round_up(group_count, 16)


def split_two(value):
    high = value.astype(jnp.bfloat16)
    return high, (value - high.astype(jnp.float32)).astype(jnp.bfloat16)


def pack_kernel(me_ref, particles_ref, classes_ref, ctf_ref, sigma_ref, shell_ref, table_ref,
                group_ref, block_ref, source_ref, index_ref):
    class_count = classes_ref.shape[0]
    particle_count, lanes = particles_ref.shape
    group_count, width = ctf_ref.shape
    rotations = table_ref.shape[0]
    levels = sigma_ref.shape[1]
    weighted_at, inverse_at, power_at, rows = row_plan(
        class_count, particle_count, rotations, group_count)
    pick_shell = (lax.broadcasted_iota(jnp.int32, (levels, width), 0) == shell_ref[...])
    sigma = lax.dot_general(sigma_ref[...], pick_shell.astype(jnp.float32),
                            (((1,), (0,)), ((), ())), precision=HIGHEST,
                            preferred_element_type=jnp.float32)
    weight = 1.0 / sigma
    weight = jnp.concatenate([weight, weight], axis=1)
    pick_group = (lax.broadcasted_iota(jnp.int32, (group_count, particle_count), 0)
                  == group_ref[...]).astype(jnp.float32)
    ctf = ctf_ref[...]
    ctf_two = jnp.concatenate([ctf, ctf], axis=1)
    ctf_part = lax.dot_general(pick_group, ctf_two, (((0,), (0,)), ((), ())), precision=HIGHEST,
                               preferred_element_type=jnp.float32)
    steps = lax.broadcasted_iota(jnp.int32, (group_count, lanes), 0).astype(jnp.float32)
    index_ref[...] = lax.dot_general(pick_group, steps, (((0,), (0,)), ((), ())), precision=HIGHEST,
                                     preferred_element_type=jnp.float32).astype(jnp.int32)
    values = particles_ref[...].astype(jnp.float32)
    source_ref[:, :lanes] = (ctf_part * values).astype(jnp.bfloat16)
    source_ref[:, lanes:] = (ctf_part * ctf_part).astype(jnp.bfloat16)
    block_ref[:class_count] = classes_ref[...]
    block_ref[weighted_at:weighted_at + particle_count] = (
        (weight * ctf_part) * values).astype(jnp.bfloat16)
    table = table_ref[...] - me_ref[0] * width
    lane = lax.broadcasted_iota(jnp.int32, (rotations, lanes), 1)
    upper = lane >= width
    target = jnp.where(upper, lane - width, lane)
    inverse = jnp.where(upper, width, 0)
    for c in range(width):
        inverse = inverse + jnp.where(table[:, c:c + 1] == target, c, 0)
    block_ref[inverse_at:inverse_at + rotations] = inverse.astype(jnp.float32).astype(jnp.bfloat16)
    high, low = split_two(weight * ctf_two * ctf_two)
    both = jnp.concatenate([high.astype(jnp.float32)[:, :width], low.astype(jnp.float32)[:, :width]], axis=1)
    pad = rows - power_at - group_count
    if pad:
        both = jnp.concatenate([both, jnp.zeros((pad, lanes), jnp.float32)], axis=0)
    block_ref[power_at:rows] = both.astype(jnp.bfloat16)


def permute_lanes(values, index_row):
    index = jnp.broadcast_to(index_row, values.shape)
    return jnp.take_along_axis(values, index, axis=1, mode="promise_in_bounds")


def main_kernel(sizes, counts, step, *refs):
    class_count, particle_count, rotations, group_count, width = counts
    lanes = 2 * width
    me_ref, index_ref, source_ref = refs[:3]
    pieces = refs[3:3 + len(sizes)]
    out_ref, log_ref = refs[3 + len(sizes):5 + len(sizes)]
    (class_all, power_all, weighted_all, table_all, turned, turned_power,
     penalty_all, score_all, post_all, source_turned) = refs[5 + len(sizes):]
    weighted_at, inverse_at, power_at, rows = row_plan(*counts[:4])
    blocks = sum(sizes)
    me = me_ref[0]
    nt = (((1,), (1,)), ((), ()))

    def slot_of(position):
        return pl.multiple_of((me ^ position) * lanes, lanes)

    def load(piece, b, position):
        at = slot_of(position)
        tile = piece[b, 0:class_count]
        class_all[:, pl.ds(at, lanes)] = tile
        weighted_all[position] = piece[b, weighted_at:weighted_at + particle_count].astype(jnp.float32)
        table = piece[b, inverse_at:inverse_at + rotations].astype(jnp.float32).astype(jnp.int32)
        table_all[position] = table
        power_all[position] = piece[b, power_at:rows].astype(jnp.float32)[:group_count]

    position = 0
    for piece, size in zip(pieces, sizes):
        if size <= 8:
            for b in range(size):
                load(piece, b, position + b)
        else:
            start = position

            def load_step(b, carry, piece=piece, start=start):
                load(piece, b, start + b)
                return carry

            lax.fori_loop(0, size, load_step, 0)
        position += size

    def penalty_step(slot):
        position = me ^ slot
        tile = class_all[:, pl.ds(pl.multiple_of(slot * lanes, lanes), lanes)].astype(jnp.float32)
        square = tile * tile
        high, low = split_two(square + pltpu.roll(square, width, 1))
        values = power_all[position]
        for r in range(rotations):
            turned_power[r * group_count:(r + 1) * group_count, :] = permute_lanes(
                values, table_all[position, r:r + 1, :])
        turned_low = turned_power[...].astype(jnp.bfloat16)
        penalty_all[...] += 0.5 * lax.dot_general(
            jnp.concatenate([turned_low, turned_low], axis=1), jnp.concatenate([high, low], axis=1),
            nt, preferred_element_type=jnp.float32)

    penalty_all[...] = jnp.zeros_like(penalty_all)
    lax.fori_loop(0, blocks, lambda slot, c: (penalty_step(slot), c)[1], 0)

    def turn(position, first):
        values = weighted_all[position]
        at = slot_of(position)
        for r in range(step):
            row = table_all[position, pl.ds(first + r, 1), :]
            turned[r * particle_count:(r + 1) * particle_count, pl.ds(at, lanes)] = permute_lanes(
                values, row).astype(jnp.bfloat16)

    group_index = jnp.concatenate([index_ref[...]] * (class_count // lanes), axis=1)

    def score_step(i, peak):
        first = i * step
        if blocks <= 8:
            for position in range(blocks):
                turn(position, first)
        else:
            lax.fori_loop(0, blocks, lambda p, c: (turn(p, first), c)[1], 0)
        cross = lax.dot_general(turned[...], class_all[...], nt, preferred_element_type=jnp.float32)
        for r in range(step):
            at = pl.multiple_of((first + r) * group_count, group_count)
            penalty = penalty_all[pl.ds(at, group_count), :]
            parts = []
            for s in range(0, particle_count, group_count):
                parts.append(jnp.take_along_axis(
                    penalty, group_index[s:s + group_count], axis=0, mode="promise_in_bounds"))
            score = cross[r * particle_count:(r + 1) * particle_count] - jnp.concatenate(parts, axis=0)
            score_all[pl.ds(pl.multiple_of((first + r) * particle_count, particle_count), particle_count), :] = score
            peak = jnp.maximum(peak, score)
        return peak

    peak = lax.fori_loop(0, rotations // step, score_step,
                         jnp.full((particle_count, class_count), -jnp.inf, jnp.float32))
    peak = jnp.max(peak, axis=1, keepdims=True)

    def exp_step(r, total):
        at = pl.multiple_of(r * particle_count, particle_count)
        value = jnp.exp(score_all[pl.ds(at, particle_count), :] - peak)
        score_all[pl.ds(at, particle_count), :] = value
        return total + value

    total = lax.fori_loop(0, rotations, exp_step,
                          jnp.zeros((particle_count, class_count), jnp.float32), unroll=2)
    total = jnp.sum(total, axis=1, keepdims=True)
    log_ref[...] = jnp.broadcast_to(peak + jnp.log(total), log_ref.shape)
    scale = 1.0 / total

    sources = source_ref[...].astype(jnp.float32)

    def sum_step(i, carry):
        first = i * step
        for r in range(step):
            at = pl.multiple_of((first + r) * particle_count, particle_count)
            here = slice(r * particle_count, (r + 1) * particle_count)
            post_all[here] = (score_all[pl.ds(at, particle_count), :] * scale).astype(jnp.bfloat16)
            row = table_all[0, pl.ds(first + r, 1), :]
            source_turned[here, :lanes] = permute_lanes(sources[:, :lanes], row).astype(jnp.bfloat16)
            source_turned[here, lanes:] = permute_lanes(sources[:, lanes:], row).astype(jnp.bfloat16)
        part = lax.dot_general(post_all[...], source_turned[...], (((0,), (0,)), ((), ())),
                               preferred_element_type=jnp.float32)
        out_ref[...] += part
        return carry

    out_ref[...] = jnp.zeros_like(out_ref)
    lax.fori_loop(0, rotations // step, sum_step, 0)


def add_kernel(left_ref, right_ref, sums_ref, weights_ref):
    lanes = sums_ref.shape[1]
    width = weights_ref.shape[1]
    sums_ref[...] = left_ref[:, :lanes] + right_ref[:, :lanes]
    weights_ref[...] = left_ref[:, lanes:lanes + width] + right_ref[:, lanes:lanes + width]


def build(mesh):
    shards = mesh.shape["shell"]
    halves = mesh.shape["batch"]

    def body(particles, classes, ctf, sigma2, shell_of, rot_table, ctf_group):
        width = shell_of.shape[0]
        lanes = 2 * width
        class_count = classes.shape[0]
        particle_count = particles.shape[0]
        rotations = rot_table.shape[0]
        group_count = ctf.shape[0]
        counts = (class_count, particle_count, rotations, group_count, width)
        rows = row_plan(*counts[:4])[3]
        vmem = pl.BlockSpec(memory_space=pltpu.VMEM)
        smem = pl.BlockSpec(memory_space=pltpu.SMEM)
        me = lax.axis_index("shell").astype(jnp.int32).reshape(1)
        block, sources, group_index = pl.pallas_call(
            pack_kernel,
            out_shape=(
                jax.ShapeDtypeStruct((rows, lanes), jnp.bfloat16),
                jax.ShapeDtypeStruct((particle_count, 2 * lanes), jnp.bfloat16),
                jax.ShapeDtypeStruct((particle_count, lanes), jnp.int32),
            ),
            in_specs=[smem] + [vmem] * 7,
            out_specs=(vmem, vmem, vmem),
            name="pack",
        )(me, particles, classes, ctf, sigma2[None], shell_of[None], rot_table, ctf_group[None])
        pieces = [block[None]]
        reach = 1
        while reach < shards:
            held = pieces[0] if len(pieces) == 1 else jnp.concatenate(pieces, axis=0)
            pieces.append(lax.ppermute(held, "shell", [(i, i ^ reach) for i in range(shards)]))
            reach *= 2
        sizes = tuple(piece.shape[0] for piece in pieces)
        blocks = sum(sizes)
        step = 8
        while step > 1 and (rotations % step or step * particle_count * blocks * lanes > 8 * 2 ** 20):
            step //= 2
        total = blocks * lanes
        part, log_rows = pl.pallas_call(
            lambda *refs: main_kernel(sizes, counts, step, *refs),
            out_shape=(
                jax.ShapeDtypeStruct((class_count, 2 * lanes), jnp.float32),
                jax.ShapeDtypeStruct((particle_count, lanes), jnp.float32),
            ),
            in_specs=[smem] + [vmem] * (2 + len(pieces)),
            out_specs=(vmem, vmem),
            scratch_shapes=[
                pltpu.VMEM((class_count, total), jnp.bfloat16),
                pltpu.VMEM((blocks, group_count, lanes), jnp.float32),
                pltpu.VMEM((blocks, particle_count, lanes), jnp.float32),
                pltpu.VMEM((blocks, rotations, lanes), jnp.int32),
                pltpu.VMEM((step * particle_count, total), jnp.bfloat16),
                pltpu.VMEM((rotations * group_count, lanes), jnp.float32),
                pltpu.VMEM((rotations * group_count, class_count), jnp.float32),
                pltpu.VMEM((rotations * particle_count, class_count), jnp.float32),
                pltpu.VMEM((step * particle_count, class_count), jnp.bfloat16),
                pltpu.VMEM((step * particle_count, 2 * lanes), jnp.bfloat16),
            ],
            name="score",
        )(me, group_index, sources, *pieces)
        other = lax.ppermute(part, "batch", [(i, halves - 1 - i) for i in range(halves)])
        class_sums, class_weights = pl.pallas_call(
            add_kernel,
            out_shape=(
                jax.ShapeDtypeStruct((class_count, lanes), jnp.float32),
                jax.ShapeDtypeStruct((class_count, width), jnp.float32),
            ),
            in_specs=[vmem, vmem],
            out_specs=(vmem, vmem),
            name="add",
        )(part, other)
        return class_sums, class_weights, log_rows[:, 0]

    return body


def solution(mesh):
    in_specs = (
        P(("groups", "batch"), "shell"),
        P("groups", "shell"),
        P("groups", "shell"),
        P("groups"),
        P("shell"),
        P(None, "shell"),
        P(("groups", "batch")),
    )
    out_specs = (P("groups", "shell"), P("groups", "shell"), P(("groups", "batch")))
    return jax.shard_map(build(mesh), mesh=mesh, in_specs=in_specs, out_specs=out_specs, check_vma=False)
```

```python
import jax
import jax.numpy as jnp
from jax import lax
from jax.experimental import pallas as pl
from jax.experimental.pallas import tpu as pltpu
from jax.sharding import PartitionSpec as P

HIGHEST = lax.Precision.HIGHEST


def round_up(value, step):
    return -(-value // step) * step


def row_plan(class_count, particle_count, rotations, group_count, halves):
    class_rows = class_count // halves
    tail_rows = round_up(rotations // 2 + group_count, 16 * halves) // halves
    shared_rows = class_rows + tail_rows
    return class_rows, tail_rows, shared_rows, shared_rows + particle_count


def split_two(value):
    high = value.astype(jnp.bfloat16)
    return high, (value - high.astype(jnp.float32)).astype(jnp.bfloat16)


def pack_kernel(halves, me_ref, core_ref, particles_ref, classes_ref, ctf_ref, sigma_ref, shell_ref,
                table_ref, group_ref, block_ref, twin_ref, source_ref, index_ref, tail_ref):
    class_count = classes_ref.shape[0]
    particle_count, lanes = particles_ref.shape
    group_count, width = ctf_ref.shape
    rotations = table_ref.shape[0]
    levels = sigma_ref.shape[1]
    class_rows, tail_rows, shared_rows, rows = row_plan(
        class_count, particle_count, rotations, group_count, halves)
    pick_shell = (lax.broadcasted_iota(jnp.int32, (levels, width), 0) == shell_ref[...])
    sigma = lax.dot_general(sigma_ref[...], pick_shell.astype(jnp.float32),
                            (((1,), (0,)), ((), ())), precision=HIGHEST,
                            preferred_element_type=jnp.float32)
    weight = 1.0 / sigma
    weight = jnp.concatenate([weight, weight], axis=1)
    pick_group = (lax.broadcasted_iota(jnp.int32, (group_count, particle_count), 0)
                  == group_ref[...]).astype(jnp.float32)
    ctf = ctf_ref[...]
    ctf_two = jnp.concatenate([ctf, ctf], axis=1)
    ctf_part = lax.dot_general(pick_group, ctf_two, (((0,), (0,)), ((), ())), precision=HIGHEST,
                               preferred_element_type=jnp.float32)
    steps = lax.broadcasted_iota(jnp.int32, (group_count, lanes), 0).astype(jnp.float32)
    index_ref[...] = lax.dot_general(pick_group, steps, (((0,), (0,)), ((), ())), precision=HIGHEST,
                                     preferred_element_type=jnp.float32).astype(jnp.int32)
    values = particles_ref[...].astype(jnp.float32)
    source_ref[:, :lanes] = (ctf_part * values).astype(jnp.bfloat16)
    source_ref[:, lanes:] = (ctf_part * ctf_part).astype(jnp.bfloat16)
    block_ref[shared_rows:rows] = ((weight * ctf_part) * values).astype(jnp.bfloat16)
    table = table_ref[...] - me_ref[0] * width
    lane = lax.broadcasted_iota(jnp.int32, (rotations, lanes), 1)
    upper = lane >= width
    target = jnp.where(upper, lane - width, lane)
    inverse = jnp.zeros((rotations, lanes), jnp.int32)
    for c in range(width):
        inverse = inverse + jnp.where(table[:, c:c + 1] == target, c, 0)
    inverse = inverse.astype(jnp.float32)
    paired = rotations // 2
    tail_ref[:paired] = jnp.where(upper[:paired], inverse[paired:], inverse[:paired])
    high, low = split_two(weight * ctf_two * ctf_two)
    tail_ref[paired:paired + group_count] = jnp.where(
        upper[:group_count], low.astype(jnp.float32), high.astype(jnp.float32))
    if paired + group_count < halves * tail_rows:
        tail_ref[paired + group_count:] = jnp.zeros(
            (halves * tail_rows - paired - group_count, lanes), jnp.float32)
    core = core_ref[0]
    for ref, part in ((block_ref, core), (twin_ref, 1 - core)):
        ref[:class_rows] = classes_ref[pl.ds(pl.multiple_of(part * class_rows, class_rows), class_rows), :]
        ref[class_rows:shared_rows] = tail_ref[
            pl.ds(pl.multiple_of(part * tail_rows, tail_rows), tail_rows), :].astype(jnp.bfloat16)


def permute_lanes(values, index_row):
    index = jnp.broadcast_to(index_row, values.shape)
    return jnp.take_along_axis(values, index, axis=1, mode="promise_in_bounds")


def main_kernel(sizes, counts, step, *refs):
    class_count, particle_count, rotations, group_count, width, halves = counts
    lanes = 2 * width
    me_ref, core_ref, index_ref, source_ref = refs[:4]
    pieces = refs[4:4 + len(sizes)]
    twins = refs[4 + len(sizes):4 + 2 * len(sizes)]
    out_ref, log_ref = refs[4 + 2 * len(sizes):6 + 2 * len(sizes)]
    (class_all, tail, power_all, weighted_all, table_all, turned, turned_power,
     penalty_all, score_all, post_all, source_turned) = refs[6 + 2 * len(sizes):]
    class_rows, tail_rows, shared_rows, rows = row_plan(
        class_count, particle_count, rotations, group_count, halves)
    blocks = sum(sizes)
    top = max(blocks.bit_length() - 2, 0)
    me = me_ref[0]
    core = core_ref[0]
    nt = (((1,), (1,)), ((), ()))
    paired = rotations // 2

    def offset_of(position):
        if blocks == 1:
            return position
        return ((position * 2) & (blocks - 1)) | (position >> top)

    def position_of(slot):
        offset = me ^ slot
        if blocks == 1:
            return offset
        return (offset >> 1) | ((offset & 1) << top)

    def slot_of(position):
        return pl.multiple_of((me ^ offset_of(position)) * lanes, lanes)

    def load(piece, twin, b, position):
        at = slot_of(position)
        for ref, part in ((piece, core), (twin, 1 - core)):
            class_all[pl.ds(pl.multiple_of(part * class_rows, class_rows), class_rows),
                      pl.ds(at, lanes)] = ref[b, :class_rows]
            tail[pl.ds(pl.multiple_of(part * tail_rows, tail_rows), tail_rows), :] = ref[
                b, class_rows:shared_rows].astype(jnp.float32)
        weighted_all[position] = piece[b, shared_rows:rows].astype(jnp.float32)
        first = tail[:paired].astype(jnp.int32)
        other = pltpu.roll(first, width, 1)
        upper = lax.broadcasted_iota(jnp.int32, (paired, lanes), 1) >= width
        table_all[position, :paired] = jnp.where(upper, other + width, first)
        table_all[position, paired:] = jnp.where(upper, first + width, other)
        power_all[position] = tail[paired:paired + group_count]

    position = 0
    for piece, twin, size in zip(pieces, twins, sizes):
        if size <= 8:
            for b in range(size):
                load(piece, twin, b, position + b)
        else:
            start = position

            def load_step(b, carry, piece=piece, twin=twin, start=start):
                load(piece, twin, b, start + b)
                return carry

            lax.fori_loop(0, size, load_step, 0)
        position += size

    def penalty_step(slot):
        position = position_of(slot)
        tile = class_all[:, pl.ds(pl.multiple_of(slot * lanes, lanes), lanes)].astype(jnp.float32)
        square = tile * tile
        high, low = split_two(square + pltpu.roll(square, width, 1))
        values = power_all[position]
        for r in range(rotations):
            turned_power[r * group_count:(r + 1) * group_count, :] = permute_lanes(
                values, table_all[position, r:r + 1, :])
        turned_low = turned_power[...].astype(jnp.bfloat16)
        penalty_all[...] += 0.5 * lax.dot_general(
            jnp.concatenate([turned_low, turned_low], axis=1), jnp.concatenate([high, low], axis=1),
            nt, preferred_element_type=jnp.float32)

    penalty_all[...] = jnp.zeros_like(penalty_all)
    lax.fori_loop(0, blocks, lambda slot, c: (penalty_step(slot), c)[1], 0)

    def turn(position, first):
        values = weighted_all[position]
        at = slot_of(position)
        for r in range(step):
            row = table_all[position, pl.ds(first + r, 1), :]
            turned[r * particle_count:(r + 1) * particle_count, pl.ds(at, lanes)] = permute_lanes(
                values, row).astype(jnp.bfloat16)

    group_index = jnp.concatenate([index_ref[...]] * (class_count // lanes), axis=1)

    def score_step(i, peak):
        first = i * step
        if blocks <= 8:
            for position in range(blocks):
                turn(position, first)
        else:
            lax.fori_loop(0, blocks, lambda p, c: (turn(p, first), c)[1], 0)
        cross = lax.dot_general(turned[...], class_all[...], nt, preferred_element_type=jnp.float32)
        for r in range(step):
            at = pl.multiple_of((first + r) * group_count, group_count)
            penalty = penalty_all[pl.ds(at, group_count), :]
            parts = []
            for s in range(0, particle_count, group_count):
                parts.append(jnp.take_along_axis(
                    penalty, group_index[s:s + group_count], axis=0, mode="promise_in_bounds"))
            score = cross[r * particle_count:(r + 1) * particle_count] - jnp.concatenate(parts, axis=0)
            score_all[pl.ds(pl.multiple_of((first + r) * particle_count, particle_count), particle_count), :] = score
            peak = jnp.maximum(peak, score)
        return peak

    peak = lax.fori_loop(0, rotations // step, score_step,
                         jnp.full((particle_count, class_count), -jnp.inf, jnp.float32))
    peak = jnp.max(peak, axis=1, keepdims=True)

    def exp_step(r, total):
        at = pl.multiple_of(r * particle_count, particle_count)
        value = jnp.exp(score_all[pl.ds(at, particle_count), :] - peak)
        score_all[pl.ds(at, particle_count), :] = value
        return total + value

    total = lax.fori_loop(0, rotations, exp_step,
                          jnp.zeros((particle_count, class_count), jnp.float32), unroll=2)
    total = jnp.sum(total, axis=1, keepdims=True)
    square = (particle_count, particle_count)
    diagonal = lax.broadcasted_iota(jnp.int32, square, 0) == lax.broadcasted_iota(jnp.int32, square, 1)
    log_ref[...] = jnp.sum(jnp.where(diagonal, peak + jnp.log(total), 0.0), axis=0, keepdims=True)
    scale = 1.0 / total

    sources = source_ref[...].astype(jnp.float32)

    def sum_step(i, carry):
        first = i * step
        for r in range(step):
            at = pl.multiple_of((first + r) * particle_count, particle_count)
            here = slice(r * particle_count, (r + 1) * particle_count)
            post_all[here] = (score_all[pl.ds(at, particle_count), :] * scale).astype(jnp.bfloat16)
            row = table_all[0, pl.ds(first + r, 1), :]
            source_turned[here, :lanes] = permute_lanes(sources[:, :lanes], row).astype(jnp.bfloat16)
            source_turned[here, lanes:] = permute_lanes(sources[:, lanes:], row).astype(jnp.bfloat16)
        part = lax.dot_general(post_all[...], source_turned[...], (((0,), (0,)), ((), ())),
                               preferred_element_type=jnp.float32)
        out_ref[...] += part
        return carry

    out_ref[...] = jnp.zeros_like(out_ref)
    lax.fori_loop(0, rotations // step, sum_step, 0)


def add_kernel(left_ref, right_ref, sums_ref, weights_ref):
    lanes = sums_ref.shape[1]
    width = weights_ref.shape[0]
    sums_ref[...] = left_ref[:, :lanes] + right_ref[:, :lanes]
    weights_ref[...] = jnp.transpose(left_ref[:, lanes:] + right_ref[:, lanes:])[:width]


def build(mesh):
    shards = mesh.shape["shell"]
    halves = mesh.shape["batch"]

    def body(particles, classes, ctf, sigma2, shell_of, rot_table, ctf_group):
        width = shell_of.shape[0]
        lanes = 2 * width
        class_count = classes.shape[0]
        particle_count = particles.shape[0]
        rotations = rot_table.shape[0]
        group_count = ctf.shape[0]
        counts = (class_count, particle_count, rotations, group_count, width, halves)
        class_rows, tail_rows, shared_rows, rows = row_plan(
            class_count, particle_count, rotations, group_count, halves)
        vmem = pl.BlockSpec(memory_space=pltpu.VMEM)
        smem = pl.BlockSpec(memory_space=pltpu.SMEM)
        me = lax.axis_index("shell").astype(jnp.int32).reshape(1)
        core = lax.axis_index("batch").astype(jnp.int32).reshape(1)
        block, twin, sources, group_index = pl.pallas_call(
            lambda *refs: pack_kernel(halves, *refs),
            out_shape=(
                jax.ShapeDtypeStruct((rows, lanes), jnp.bfloat16),
                jax.ShapeDtypeStruct((shared_rows, lanes), jnp.bfloat16),
                jax.ShapeDtypeStruct((particle_count, 2 * lanes), jnp.bfloat16),
                jax.ShapeDtypeStruct((particle_count, lanes), jnp.int32),
            ),
            in_specs=[smem] * 2 + [vmem] * 7,
            out_specs=(vmem, vmem, vmem, vmem),
            scratch_shapes=[pltpu.VMEM((halves * tail_rows, lanes), jnp.float32)],
            name="pack",
        )(me, core, particles, classes, ctf, sigma2[None], shell_of[None], rot_table, ctf_group[None])
        swap = [(i, halves - 1 - i) for i in range(halves)]
        pieces, twins = [block[None]], [twin[None]]
        reaches = [2 ** i for i in range(1, shards.bit_length() - 1)] + [1]
        for reach in reaches if shards > 1 else ():
            held = pieces[0] if len(pieces) == 1 else jnp.concatenate(pieces, axis=0)
            pieces.append(lax.ppermute(held, "shell", [(i, i ^ reach) for i in range(shards)]))
            twins.append(lax.ppermute(pieces[-1], "batch", swap))
        sizes = tuple(piece.shape[0] for piece in pieces)
        blocks = sum(sizes)
        step = 8
        while step > 1 and (rotations % step or step * particle_count * blocks * lanes > 8 * 2 ** 20):
            step //= 2
        total = blocks * lanes
        part, log_rows = pl.pallas_call(
            lambda *refs: main_kernel(sizes, counts, step, *refs),
            out_shape=(
                jax.ShapeDtypeStruct((class_count, 2 * lanes), jnp.float32),
                jax.ShapeDtypeStruct((1, particle_count), jnp.float32),
            ),
            in_specs=[smem] * 2 + [vmem] * (2 + 2 * len(pieces)),
            out_specs=(vmem, vmem),
            scratch_shapes=[
                pltpu.VMEM((class_count, total), jnp.bfloat16),
                pltpu.VMEM((halves * tail_rows, lanes), jnp.float32),
                pltpu.VMEM((blocks, group_count, lanes), jnp.float32),
                pltpu.VMEM((blocks, particle_count, lanes), jnp.float32),
                pltpu.VMEM((blocks, rotations, lanes), jnp.int32),
                pltpu.VMEM((step * particle_count, total), jnp.bfloat16),
                pltpu.VMEM((rotations * group_count, lanes), jnp.float32),
                pltpu.VMEM((rotations * group_count, class_count), jnp.float32),
                pltpu.VMEM((rotations * particle_count, class_count), jnp.float32),
                pltpu.VMEM((step * particle_count, class_count), jnp.bfloat16),
                pltpu.VMEM((step * particle_count, 2 * lanes), jnp.bfloat16),
            ],
            name="score",
        )(me, core, group_index, sources, *pieces, *twins)
        other = lax.ppermute(part, "batch", swap)
        class_sums, class_weights = pl.pallas_call(
            add_kernel,
            out_shape=(
                jax.ShapeDtypeStruct((class_count, lanes), jnp.float32),
                jax.ShapeDtypeStruct((width, class_count), jnp.float32),
            ),
            in_specs=[vmem, vmem],
            out_specs=(vmem, vmem),
            name="add",
        )(part, other)
        return class_sums, class_weights.T, log_rows[0]

    return body


def solution(mesh):
    in_specs = (
        P(("groups", "batch"), "shell"),
        P("groups", "shell"),
        P("groups", "shell"),
        P("groups"),
        P("shell"),
        P(None, "shell"),
        P(("groups", "batch")),
    )
    out_specs = (P("groups", "shell"), P("groups", "shell"), P(("groups", "batch")))
    return jax.shard_map(build(mesh), mesh=mesh, in_specs=in_specs, out_specs=out_specs, check_vma=False)
```

```python
import jax
import jax.numpy as jnp
from jax import lax
from jax.experimental import pallas as pl
from jax.experimental.pallas import tpu as pltpu
from jax.sharding import PartitionSpec as P

HIGHEST = lax.Precision.HIGHEST


def round_up(value, step):
    return -(-value // step) * step


def row_plan(class_count, particle_count, rotations, group_count, halves):
    class_rows = class_count // halves
    tail_rows = round_up(rotations // 2 + group_count, 16 * halves) // halves
    shared_rows = class_rows + tail_rows
    return class_rows, tail_rows, shared_rows, shared_rows + particle_count


def split_two(value):
    high = value.astype(jnp.bfloat16)
    return high, (value - high.astype(jnp.float32)).astype(jnp.bfloat16)


def pack_kernel(halves, me_ref, core_ref, particles_ref, classes_ref, ctf_ref, sigma_ref, shell_ref,
                table_ref, group_ref, block_ref, twin_ref, source_ref, index_ref, tail_ref):
    class_count = classes_ref.shape[0]
    particle_count, lanes = particles_ref.shape
    group_count, width = ctf_ref.shape
    rotations = table_ref.shape[0]
    levels = sigma_ref.shape[1]
    class_rows, tail_rows, shared_rows, rows = row_plan(
        class_count, particle_count, rotations, group_count, halves)
    pick_shell = (lax.broadcasted_iota(jnp.int32, (levels, width), 0) == shell_ref[...])
    sigma = lax.dot_general(sigma_ref[...], pick_shell.astype(jnp.float32),
                            (((1,), (0,)), ((), ())), precision=HIGHEST,
                            preferred_element_type=jnp.float32)
    weight = 1.0 / sigma
    weight = jnp.concatenate([weight, weight], axis=1)
    pick_group = (lax.broadcasted_iota(jnp.int32, (group_count, particle_count), 0)
                  == group_ref[...]).astype(jnp.float32)
    ctf = ctf_ref[...]
    ctf_two = jnp.concatenate([ctf, ctf], axis=1)
    ctf_part = lax.dot_general(pick_group, ctf_two, (((0,), (0,)), ((), ())), precision=HIGHEST,
                               preferred_element_type=jnp.float32)
    steps = lax.broadcasted_iota(jnp.int32, (group_count, lanes), 0).astype(jnp.float32)
    index_ref[...] = lax.dot_general(pick_group, steps, (((0,), (0,)), ((), ())), precision=HIGHEST,
                                     preferred_element_type=jnp.float32).astype(jnp.int32)
    values = particles_ref[...].astype(jnp.float32)
    source_ref[:, :lanes] = (ctf_part * values).astype(jnp.bfloat16)
    source_ref[:, lanes:] = (ctf_part * ctf_part).astype(jnp.bfloat16)
    block_ref[shared_rows:rows] = ((weight * ctf_part) * values).astype(jnp.bfloat16)
    table = table_ref[...] - me_ref[0] * width
    lane = lax.broadcasted_iota(jnp.int32, (rotations, lanes), 1)
    upper = lane >= width
    target = jnp.where(upper, lane - width, lane)
    inverse = jnp.zeros((rotations, lanes), jnp.int32)
    for c in range(width):
        inverse = inverse + jnp.where(table[:, c:c + 1] == target, c, 0)
    inverse = inverse.astype(jnp.float32)
    paired = rotations // 2
    tail_ref[:paired] = jnp.where(upper[:paired], inverse[paired:], inverse[:paired])
    high, low = split_two(weight * ctf_two * ctf_two)
    tail_ref[paired:paired + group_count] = jnp.where(
        upper[:group_count], low.astype(jnp.float32), high.astype(jnp.float32))
    if paired + group_count < halves * tail_rows:
        tail_ref[paired + group_count:] = jnp.zeros(
            (halves * tail_rows - paired - group_count, lanes), jnp.float32)
    core = core_ref[0]
    for ref, part in ((block_ref, core), (twin_ref, 1 - core)):
        ref[:class_rows] = classes_ref[pl.ds(pl.multiple_of(part * class_rows, class_rows), class_rows), :]
        ref[class_rows:shared_rows] = tail_ref[
            pl.ds(pl.multiple_of(part * tail_rows, tail_rows), tail_rows), :].astype(jnp.bfloat16)


def permute_lanes(values, index_row):
    index = jnp.broadcast_to(index_row, values.shape)
    return jnp.take_along_axis(values, index, axis=1, mode="promise_in_bounds")


NT = (((1,), (1,)), ((), ()))


def half_scores(counts, step, me, core, index_ref, pieces, twins, scratch, finish):
    class_count, particle_count, rotations, group_count, width, halves = counts
    lanes = 2 * width
    (class_all, tail, power_all, weighted_all, table_all, turned, turned_power, penalty_all) = scratch
    class_rows, tail_rows, shared_rows, rows = row_plan(
        class_count, particle_count, rotations, group_count, halves)
    blocks = sum(piece.shape[0] for piece in pieces)
    paired = rotations // 2
    base = me >> 1

    def load(piece, twin, b, position):
        at = pl.multiple_of((base ^ position) * lanes, lanes)
        for ref, part in ((piece, core), (twin, 1 - core)):
            class_all[pl.ds(pl.multiple_of(part * class_rows, class_rows), class_rows),
                      pl.ds(at, lanes)] = ref[b, :class_rows]
            tail[pl.ds(pl.multiple_of(part * tail_rows, tail_rows), tail_rows), :] = ref[
                b, class_rows:shared_rows].astype(jnp.float32)
        weighted_all[position] = piece[b, shared_rows:rows].astype(jnp.float32)
        first = tail[:paired].astype(jnp.int32)
        other = pltpu.roll(first, width, 1)
        upper = lax.broadcasted_iota(jnp.int32, (paired, lanes), 1) >= width
        table_all[position, :paired] = jnp.where(upper, other + width, first)
        table_all[position, paired:] = jnp.where(upper, first + width, other)
        power_all[position] = tail[paired:paired + group_count]

    position = 0
    for piece, twin in zip(pieces, twins):
        size = piece.shape[0]
        if size <= 8:
            for b in range(size):
                load(piece, twin, b, position + b)
        else:
            start = position

            def load_step(b, carry, piece=piece, twin=twin, start=start):
                load(piece, twin, b, start + b)
                return carry

            lax.fori_loop(0, size, load_step, 0)
        position += size

    def penalty_step(slot):
        position = base ^ slot
        tile = class_all[:, pl.ds(pl.multiple_of(slot * lanes, lanes), lanes)].astype(jnp.float32)
        square = tile * tile
        high, low = split_two(square + pltpu.roll(square, width, 1))
        values = power_all[position]
        for r in range(rotations):
            turned_power[r * group_count:(r + 1) * group_count, :] = permute_lanes(
                values, table_all[position, r:r + 1, :])
        turned_low = turned_power[...].astype(jnp.bfloat16)
        penalty_all[...] += 0.5 * lax.dot_general(
            jnp.concatenate([turned_low, turned_low], axis=1), jnp.concatenate([high, low], axis=1),
            NT, preferred_element_type=jnp.float32)

    penalty_all[...] = jnp.zeros_like(penalty_all)
    lax.fori_loop(0, blocks, lambda slot, c: (penalty_step(slot), c)[1], 0)

    def turn(position, first):
        values = weighted_all[position]
        at = pl.multiple_of((base ^ position) * lanes, lanes)
        for r in range(step):
            row = table_all[position, pl.ds(first + r, 1), :]
            turned[r * particle_count:(r + 1) * particle_count, pl.ds(at, lanes)] = permute_lanes(
                values, row).astype(jnp.bfloat16)

    group_index = jnp.concatenate([index_ref[...]] * (class_count // lanes), axis=1)

    def score_step(i, carry):
        first = i * step
        if blocks <= 8:
            for position in range(blocks):
                turn(position, first)
        else:
            lax.fori_loop(0, blocks, lambda p, c: (turn(p, first), c)[1], 0)
        cross = lax.dot_general(turned[...], class_all[...], NT, preferred_element_type=jnp.float32)
        carry = finish(i, None, None, carry)
        for r in range(step):
            at = pl.multiple_of((first + r) * group_count, group_count)
            penalty = penalty_all[pl.ds(at, group_count), :]
            parts = []
            for s in range(0, particle_count, group_count):
                parts.append(jnp.take_along_axis(
                    penalty, group_index[s:s + group_count], axis=0, mode="promise_in_bounds"))
            score = cross[r * particle_count:(r + 1) * particle_count] - jnp.concatenate(parts, axis=0)
            carry = finish(i, r, score, carry)
        return carry

    return score_step


def early_kernel(size, counts, step, *refs):
    me_ref, core_ref, index_ref = refs[:3]
    pieces, twins = refs[3:3 + size], refs[3 + size:3 + 2 * size]
    score_out = refs[3 + 2 * size]
    scratch, (stage, sem) = refs[4 + 2 * size:-2], refs[-2:]
    particle_count, rotations = counts[1:3]
    chunk = step * particle_count

    def copy(i):
        return pltpu.make_async_copy(stage.at[pl.ds(i * chunk, chunk)],
                                     score_out.at[pl.ds(i * chunk, chunk)], sem.at[i])

    def finish(i, r, score, carry):
        if score is not None:
            at = pl.multiple_of((i * step + r) * particle_count, particle_count)
            stage[pl.ds(at, particle_count), :] = score
            if r == step - 1:
                copy(i).start()
        return carry

    score_step = half_scores(counts, step, me_ref[0], core_ref[0], index_ref, pieces, twins, scratch, finish)
    lax.fori_loop(0, rotations // step, score_step, 0)
    for i in range(rotations // step):
        copy(i).wait()


def main_kernel(counts, step, *refs):
    class_count, particle_count, rotations, group_count, width, halves = counts
    lanes = 2 * width
    (me_ref, core_ref, index_ref, source_ref, block_ref, block_twin_ref, piece_ref, twin_ref, early_ref,
     sums_ref, weights_ref, log_ref) = refs[:12]
    scratch, (early, score_all, own_table, post_all, source_turned, total_all, sem) = refs[12:-7], refs[-7:]
    table_all = scratch[4]
    chunk = step * particle_count

    def copy(i):
        return pltpu.make_async_copy(early_ref.at[pl.ds(i * chunk, chunk)],
                                     early.at[pl.ds(i * chunk, chunk)], sem.at[i])

    for i in range(rotations // step):
        copy(i).start()

    def finish(i, r, score, peak):
        if score is None:
            copy(i).wait()
            return peak
        at = pl.multiple_of((i * step + r) * particle_count, particle_count)
        score = score + early[pl.ds(at, particle_count), :]
        score_all[pl.ds(at, particle_count), :] = score
        return jnp.maximum(peak, score)

    class_rows, tail_rows, shared_rows, rows = row_plan(
        class_count, particle_count, rotations, group_count, halves)
    score_step = half_scores(counts, step, me_ref[0], core_ref[0], index_ref, (piece_ref,), (twin_ref,),
                             scratch, finish)
    peak = lax.fori_loop(0, rotations // step, score_step,
                         jnp.full((particle_count, class_count), -jnp.inf, jnp.float32))
    peak = jnp.max(peak, axis=1, keepdims=True)

    def exp_step(r, total):
        at = pl.multiple_of(r * particle_count, particle_count)
        value = jnp.exp(score_all[pl.ds(at, particle_count), :] - peak)
        score_all[pl.ds(at, particle_count), :] = value
        return total + value

    total = lax.fori_loop(0, rotations, exp_step,
                          jnp.zeros((particle_count, class_count), jnp.float32), unroll=2)
    total = jnp.sum(total, axis=1, keepdims=True)
    square = (particle_count, particle_count)
    diagonal = lax.broadcasted_iota(jnp.int32, square, 0) == lax.broadcasted_iota(jnp.int32, square, 1)
    log_ref[...] = jnp.sum(jnp.where(diagonal, peak + jnp.log(total), 0.0), axis=0, keepdims=True)
    scale = 1.0 / total

    core = core_ref[0]
    paired = rotations // 2
    tail = scratch[1]
    for ref, part in ((block_ref, core), (block_twin_ref, 1 - core)):
        tail[pl.ds(pl.multiple_of(part * tail_rows, tail_rows), tail_rows), :] = ref[
            0, class_rows:shared_rows].astype(jnp.float32)
    first_rows = tail[:paired].astype(jnp.int32)
    other_rows = pltpu.roll(first_rows, width, 1)
    upper = lax.broadcasted_iota(jnp.int32, (paired, lanes), 1) >= width
    own_table[:paired] = jnp.where(upper, other_rows + width, first_rows)
    own_table[paired:] = jnp.where(upper, first_rows + width, other_rows)
    sources = source_ref[...].astype(jnp.float32)

    def sum_step(i, carry):
        first = i * step
        for r in range(step):
            at = pl.multiple_of((first + r) * particle_count, particle_count)
            here = slice(r * particle_count, (r + 1) * particle_count)
            post_all[here] = (score_all[pl.ds(at, particle_count), :] * scale).astype(jnp.bfloat16)
            row = own_table[pl.ds(first + r, 1), :]
            source_turned[here, :lanes] = permute_lanes(sources[:, :lanes], row).astype(jnp.bfloat16)
            source_turned[here, lanes:] = permute_lanes(sources[:, lanes:], row).astype(jnp.bfloat16)
        total_all[...] += lax.dot_general(source_turned[...], post_all[...], (((0,), (0,)), ((), ())),
                                          preferred_element_type=jnp.float32)
        return carry

    total_all[...] = jnp.zeros_like(total_all)
    lax.fori_loop(0, rotations // step, sum_step, 0)
    sums_ref[...] = jnp.transpose(total_all[:lanes])
    weights_ref[...] = total_all[lanes:lanes + width]


def build(mesh):
    shards = mesh.shape["shell"]
    halves = mesh.shape["batch"]

    def body(particles, classes, ctf, sigma2, shell_of, rot_table, ctf_group):
        width = shell_of.shape[0]
        lanes = 2 * width
        class_count = classes.shape[0]
        particle_count = particles.shape[0]
        rotations = rot_table.shape[0]
        group_count = ctf.shape[0]
        counts = (class_count, particle_count, rotations, group_count, width, halves)
        class_rows, tail_rows, shared_rows, rows = row_plan(
            class_count, particle_count, rotations, group_count, halves)
        vmem = pl.BlockSpec(memory_space=pltpu.VMEM)
        smem = pl.BlockSpec(memory_space=pltpu.SMEM)
        me = lax.axis_index("shell").astype(jnp.int32).reshape(1)
        core = lax.axis_index("batch").astype(jnp.int32).reshape(1)
        block, twin, sources, group_index = pl.pallas_call(
            lambda *refs: pack_kernel(halves, *refs),
            out_shape=(
                jax.ShapeDtypeStruct((rows, lanes), jnp.bfloat16),
                jax.ShapeDtypeStruct((shared_rows, lanes), jnp.bfloat16),
                jax.ShapeDtypeStruct((particle_count, 2 * lanes), jnp.bfloat16),
                jax.ShapeDtypeStruct((particle_count, lanes), jnp.int32),
            ),
            in_specs=[smem] * 2 + [vmem] * 7,
            out_specs=(vmem, vmem, vmem, vmem),
            scratch_shapes=[pltpu.VMEM((halves * tail_rows, lanes), jnp.float32)],
            name="pack",
        )(me, core, particles, classes, ctf, sigma2[None], shell_of[None], rot_table, ctf_group[None])
        swap = [(i, halves - 1 - i) for i in range(halves)]
        pieces, twins = [block[None]], [twin[None]]
        reaches = [2 ** i for i in range(1, shards.bit_length() - 1)] + [1]
        for reach in reaches if shards > 1 else ():
            held = pieces[0] if len(pieces) == 1 else jnp.concatenate(pieces, axis=0)
            pieces.append(lax.ppermute(held, "shell", [(i, i ^ reach) for i in range(shards)]))
            if len(pieces) <= len(reaches):
                twins.append(lax.ppermute(pieces[-1], "batch", swap))
        blocks = shards // 2
        step = 8
        while step > 1 and (rotations % step or step * particle_count * blocks * lanes > 4 * 2 ** 20):
            step //= 2
        total = blocks * lanes
        score_rows = rotations * particle_count
        half_scratch = [
            pltpu.VMEM((class_count, total), jnp.bfloat16),
            pltpu.VMEM((halves * tail_rows, lanes), jnp.float32),
            pltpu.VMEM((blocks, group_count, lanes), jnp.float32),
            pltpu.VMEM((blocks, particle_count, lanes), jnp.float32),
            pltpu.VMEM((blocks, rotations, lanes), jnp.int32),
            pltpu.VMEM((step * particle_count, total), jnp.bfloat16),
            pltpu.VMEM((rotations * group_count, lanes), jnp.float32),
            pltpu.VMEM((rotations * group_count, class_count), jnp.float32),
        ]
        held_back = pl.BlockSpec(memory_space=pl.ANY)
        size = len(pieces) - 1
        early = pl.pallas_call(
            lambda *refs: early_kernel(size, counts, step, *refs),
            out_shape=jax.ShapeDtypeStruct((score_rows, class_count), jnp.float32),
            in_specs=[smem] * 2 + [vmem] * (1 + 2 * size),
            out_specs=held_back,
            scratch_shapes=half_scratch + [
                pltpu.VMEM((score_rows, class_count), jnp.float32),
                pltpu.SemaphoreType.DMA((rotations // step,)),
            ],
            name="early",
        )(me, core, group_index, *pieces[:-1], *twins)
        last, early = lax.optimization_barrier((pieces[-1], early))
        last_twin = lax.ppermute(last, "batch", swap)
        sums, weights, log_rows = pl.pallas_call(
            lambda *refs: main_kernel(counts, step, *refs),
            out_shape=(
                jax.ShapeDtypeStruct((class_count, lanes), jnp.float32),
                jax.ShapeDtypeStruct((width, class_count), jnp.float32),
                jax.ShapeDtypeStruct((1, particle_count), jnp.float32),
            ),
            in_specs=[smem] * 2 + [vmem] * 6 + [held_back],
            out_specs=(vmem, vmem, vmem),
            scratch_shapes=half_scratch + [
                pltpu.VMEM((score_rows, class_count), jnp.float32),
                pltpu.VMEM((score_rows, class_count), jnp.float32),
                pltpu.VMEM((rotations, lanes), jnp.int32),
                pltpu.VMEM((step * particle_count, class_count), jnp.bfloat16),
                pltpu.VMEM((step * particle_count, 2 * lanes), jnp.bfloat16),
                pltpu.VMEM((2 * lanes, class_count), jnp.float32),
                pltpu.SemaphoreType.DMA((rotations // step,)),
            ],
            name="score",
        )(me, core, group_index, sources, pieces[0], twins[0], last, last_twin, early)
        class_sums = sums + lax.ppermute(sums, "batch", swap)
        class_weights = weights + lax.ppermute(weights, "batch", swap)
        return class_sums, class_weights.T, log_rows[0]

    return body


def solution(mesh):
    in_specs = (
        P(("groups", "batch"), "shell"),
        P("groups", "shell"),
        P("groups", "shell"),
        P("groups"),
        P("shell"),
        P(None, "shell"),
        P(("groups", "batch")),
    )
    out_specs = (P("groups", "shell"), P("groups", "shell"), P(("groups", "batch")))
    return jax.shard_map(build(mesh), mesh=mesh, in_specs=in_specs, out_specs=out_specs, check_vma=False)
```

```python
import jax
import jax.numpy as jnp
from jax import lax
from jax.experimental import pallas as pl
from jax.experimental.pallas import tpu as pltpu
from jax.sharding import PartitionSpec as P

HIGHEST = lax.Precision.HIGHEST


def round_up(value, step):
    return -(-value // step) * step


def row_plan(class_count, particle_count, rotations, group_count, halves):
    class_rows = class_count // halves
    tail_rows = round_up(rotations // 2 + group_count, 16 * halves) // halves
    shared_rows = class_rows + tail_rows
    return class_rows, tail_rows, shared_rows, shared_rows + particle_count


def split_two(value):
    high = value.astype(jnp.bfloat16)
    return high, (value - high.astype(jnp.float32)).astype(jnp.bfloat16)


def pack_kernel(halves, me_ref, core_ref, particles_ref, classes_ref, ctf_ref, sigma_ref, shell_ref,
                table_ref, group_ref, block_ref, twin_ref, source_ref, index_ref, own_ref, tail_ref):
    class_count = classes_ref.shape[0]
    particle_count, lanes = particles_ref.shape
    group_count, width = ctf_ref.shape
    rotations = table_ref.shape[0]
    levels = sigma_ref.shape[1]
    class_rows, tail_rows, shared_rows, rows = row_plan(
        class_count, particle_count, rotations, group_count, halves)
    pick_shell = (lax.broadcasted_iota(jnp.int32, (levels, width), 0) == shell_ref[...])
    sigma = lax.dot_general(sigma_ref[...], pick_shell.astype(jnp.float32),
                            (((1,), (0,)), ((), ())), precision=HIGHEST,
                            preferred_element_type=jnp.float32)
    weight = 1.0 / sigma
    weight = jnp.concatenate([weight, weight], axis=1)
    pick_group = (lax.broadcasted_iota(jnp.int32, (group_count, particle_count), 0)
                  == group_ref[...]).astype(jnp.float32)
    ctf = ctf_ref[...]
    ctf_two = jnp.concatenate([ctf, ctf], axis=1)
    ctf_part = lax.dot_general(pick_group, ctf_two, (((0,), (0,)), ((), ())), precision=HIGHEST,
                               preferred_element_type=jnp.float32)
    steps = lax.broadcasted_iota(jnp.int32, (group_count, lanes), 0).astype(jnp.float32)
    index_ref[...] = lax.dot_general(pick_group, steps, (((0,), (0,)), ((), ())), precision=HIGHEST,
                                     preferred_element_type=jnp.float32).astype(jnp.int32)
    values = particles_ref[...].astype(jnp.float32)
    source_ref[:, :lanes] = (ctf_part * values).astype(jnp.bfloat16)
    source_ref[:, lanes:] = (ctf_part * ctf_part).astype(jnp.bfloat16)
    block_ref[shared_rows:rows] = ((weight * ctf_part) * values).astype(jnp.bfloat16)
    table = table_ref[...] - me_ref[0] * width
    lane = lax.broadcasted_iota(jnp.int32, (rotations, lanes), 1)
    upper = lane >= width
    target = jnp.where(upper, lane - width, lane)
    inverse = jnp.zeros((rotations, lanes), jnp.int32)
    for c in range(width):
        inverse = inverse + jnp.where(table[:, c:c + 1] == target, c, 0)
    own_ref[...] = jnp.where(upper, inverse + width, inverse)
    inverse = inverse.astype(jnp.float32)
    paired = rotations // 2
    tail_ref[:paired] = jnp.where(upper[:paired], inverse[paired:], inverse[:paired])
    high, low = split_two(weight * ctf_two * ctf_two)
    tail_ref[paired:paired + group_count] = jnp.where(
        upper[:group_count], low.astype(jnp.float32), high.astype(jnp.float32))
    if paired + group_count < halves * tail_rows:
        tail_ref[paired + group_count:] = jnp.zeros(
            (halves * tail_rows - paired - group_count, lanes), jnp.float32)
    core = core_ref[0]
    for ref, part in ((block_ref, core), (twin_ref, 1 - core)):
        ref[:class_rows] = classes_ref[pl.ds(pl.multiple_of(part * class_rows, class_rows), class_rows), :]
        ref[class_rows:shared_rows] = tail_ref[
            pl.ds(pl.multiple_of(part * tail_rows, tail_rows), tail_rows), :].astype(jnp.bfloat16)


def permute_lanes(values, index_row):
    index = jnp.broadcast_to(index_row, values.shape)
    return jnp.take_along_axis(values, index, axis=1, mode="promise_in_bounds")


def spread_kernel(table_ref, source_ref, out_ref):
    particle_count = source_ref.shape[0]
    lanes = source_ref.shape[1] // 2
    rotations = table_ref.shape[0]
    sources = source_ref[...].astype(jnp.float32)

    def step(r, carry):
        row = table_ref[pl.ds(r, 1), :]
        at = pl.ds(pl.multiple_of(r * particle_count, particle_count), particle_count)
        out_ref[at, :lanes] = permute_lanes(sources[:, :lanes], row).astype(jnp.bfloat16)
        out_ref[at, lanes:] = permute_lanes(sources[:, lanes:], row).astype(jnp.bfloat16)
        return carry

    lax.fori_loop(0, rotations, step, 0, unroll=4)


def main_kernel(sizes, counts, step, *refs):
    class_count, particle_count, rotations, group_count, width, halves = counts
    lanes = 2 * width
    me_ref, core_ref, index_ref, source_ref = refs[:4]
    pieces = refs[4:4 + len(sizes)]
    twins = refs[4 + len(sizes):4 + 2 * len(sizes)]
    out_ref, log_ref = refs[4 + 2 * len(sizes):6 + 2 * len(sizes)]
    (class_all, tail, power_all, weighted_all, table_all, turned, turned_power,
     penalty_all, score_all, post_all, source_turned, sem) = refs[6 + 2 * len(sizes):]
    fetch = pltpu.make_async_copy(source_ref, source_turned, sem)
    fetch.start()
    class_rows, tail_rows, shared_rows, rows = row_plan(
        class_count, particle_count, rotations, group_count, halves)
    blocks = sum(sizes)
    top = max(blocks.bit_length() - 2, 0)
    me = me_ref[0]
    core = core_ref[0]
    nt = (((1,), (1,)), ((), ()))
    paired = rotations // 2

    def offset_of(position):
        if blocks == 1:
            return position
        return ((position * 2) & (blocks - 1)) | (position >> top)

    def position_of(slot):
        offset = me ^ slot
        if blocks == 1:
            return offset
        return (offset >> 1) | ((offset & 1) << top)

    def slot_of(position):
        return pl.multiple_of((me ^ offset_of(position)) * lanes, lanes)

    def load(piece, twin, b, position):
        at = slot_of(position)
        for ref, part in ((piece, core), (twin, 1 - core)):
            class_all[pl.ds(pl.multiple_of(part * class_rows, class_rows), class_rows),
                      pl.ds(at, lanes)] = ref[b, :class_rows]
            tail[pl.ds(pl.multiple_of(part * tail_rows, tail_rows), tail_rows), :] = ref[
                b, class_rows:shared_rows].astype(jnp.float32)
        weighted_all[position] = piece[b, shared_rows:rows].astype(jnp.float32)
        first = tail[:paired].astype(jnp.int32)
        other = pltpu.roll(first, width, 1)
        upper = lax.broadcasted_iota(jnp.int32, (paired, lanes), 1) >= width
        table_all[position, :paired] = jnp.where(upper, other + width, first)
        table_all[position, paired:] = jnp.where(upper, first + width, other)
        power_all[position] = tail[paired:paired + group_count]

    position = 0
    for piece, twin, size in zip(pieces, twins, sizes):
        if size <= 8:
            for b in range(size):
                load(piece, twin, b, position + b)
        else:
            start = position

            def load_step(b, carry, piece=piece, twin=twin, start=start):
                load(piece, twin, b, start + b)
                return carry

            lax.fori_loop(0, size, load_step, 0)
        position += size

    def penalty_step(slot):
        position = position_of(slot)
        tile = class_all[:, pl.ds(pl.multiple_of(slot * lanes, lanes), lanes)].astype(jnp.float32)
        square = tile * tile
        high, low = split_two(square + pltpu.roll(square, width, 1))
        values = power_all[position]
        for r in range(rotations):
            turned_power[r * group_count:(r + 1) * group_count, :] = permute_lanes(
                values, table_all[position, r:r + 1, :])
        turned_low = turned_power[...].astype(jnp.bfloat16)
        penalty_all[...] += 0.5 * lax.dot_general(
            jnp.concatenate([turned_low, turned_low], axis=1), jnp.concatenate([high, low], axis=1),
            nt, preferred_element_type=jnp.float32)

    penalty_all[...] = jnp.zeros_like(penalty_all)
    lax.fori_loop(0, blocks, lambda slot, c: (penalty_step(slot), c)[1], 0)

    def turn(position, first):
        values = weighted_all[position]
        at = slot_of(position)
        for r in range(step):
            row = table_all[position, pl.ds(first + r, 1), :]
            turned[r * particle_count:(r + 1) * particle_count, pl.ds(at, lanes)] = permute_lanes(
                values, row).astype(jnp.bfloat16)

    group_index = jnp.concatenate([index_ref[...]] * (class_count // lanes), axis=1)

    def score_step(i, peak):
        first = i * step
        if blocks <= 8:
            for position in range(blocks):
                turn(position, first)
        else:
            lax.fori_loop(0, blocks, lambda p, c: (turn(p, first), c)[1], 0)
        cross = lax.dot_general(turned[...], class_all[...], nt, preferred_element_type=jnp.float32)
        for r in range(step):
            at = pl.multiple_of((first + r) * group_count, group_count)
            penalty = penalty_all[pl.ds(at, group_count), :]
            parts = []
            for s in range(0, particle_count, group_count):
                parts.append(jnp.take_along_axis(
                    penalty, group_index[s:s + group_count], axis=0, mode="promise_in_bounds"))
            score = cross[r * particle_count:(r + 1) * particle_count] - jnp.concatenate(parts, axis=0)
            score_all[pl.ds(pl.multiple_of((first + r) * particle_count, particle_count), particle_count), :] = score
            peak = jnp.maximum(peak, score)
        return peak

    peak = lax.fori_loop(0, rotations // step, score_step,
                         jnp.full((particle_count, class_count), -jnp.inf, jnp.float32))
    peak = jnp.max(peak, axis=1, keepdims=True)

    def exp_step(r, total):
        at = pl.multiple_of(r * particle_count, particle_count)
        value = jnp.exp(score_all[pl.ds(at, particle_count), :] - peak)
        score_all[pl.ds(at, particle_count), :] = value
        return total + value

    total = lax.fori_loop(0, rotations, exp_step,
                          jnp.zeros((particle_count, class_count), jnp.float32), unroll=2)
    total = jnp.sum(total, axis=1, keepdims=True)
    square = (particle_count, particle_count)
    diagonal = lax.broadcasted_iota(jnp.int32, square, 0) == lax.broadcasted_iota(jnp.int32, square, 1)
    log_ref[...] = jnp.sum(jnp.where(diagonal, peak + jnp.log(total), 0.0), axis=0, keepdims=True)
    scale = 1.0 / total

    fetch.wait()

    def sum_step(i, carry):
        first = i * step
        for r in range(step):
            at = pl.multiple_of((first + r) * particle_count, particle_count)
            here = slice(r * particle_count, (r + 1) * particle_count)
            post_all[here] = (score_all[pl.ds(at, particle_count), :] * scale).astype(jnp.bfloat16)
        span = pl.ds(pl.multiple_of(first * particle_count, particle_count), step * particle_count)
        part = lax.dot_general(post_all[...], source_turned[span, :], (((0,), (0,)), ((), ())),
                               preferred_element_type=jnp.float32)
        out_ref[...] += part
        return carry

    out_ref[...] = jnp.zeros_like(out_ref)
    lax.fori_loop(0, rotations // step, sum_step, 0)


def add_kernel(left_ref, right_ref, sums_ref, weights_ref):
    lanes = sums_ref.shape[1]
    width = weights_ref.shape[0]
    sums_ref[...] = left_ref[:, :lanes] + right_ref[:, :lanes]
    weights_ref[...] = jnp.transpose(left_ref[:, lanes:] + right_ref[:, lanes:])[:width]


def build(mesh):
    shards = mesh.shape["shell"]
    halves = mesh.shape["batch"]

    def body(particles, classes, ctf, sigma2, shell_of, rot_table, ctf_group):
        width = shell_of.shape[0]
        lanes = 2 * width
        class_count = classes.shape[0]
        particle_count = particles.shape[0]
        rotations = rot_table.shape[0]
        group_count = ctf.shape[0]
        counts = (class_count, particle_count, rotations, group_count, width, halves)
        class_rows, tail_rows, shared_rows, rows = row_plan(
            class_count, particle_count, rotations, group_count, halves)
        vmem = pl.BlockSpec(memory_space=pltpu.VMEM)
        smem = pl.BlockSpec(memory_space=pltpu.SMEM)
        me = lax.axis_index("shell").astype(jnp.int32).reshape(1)
        core = lax.axis_index("batch").astype(jnp.int32).reshape(1)
        block, twin, sources, group_index, own_table = pl.pallas_call(
            lambda *refs: pack_kernel(halves, *refs),
            out_shape=(
                jax.ShapeDtypeStruct((rows, lanes), jnp.bfloat16),
                jax.ShapeDtypeStruct((shared_rows, lanes), jnp.bfloat16),
                jax.ShapeDtypeStruct((particle_count, 2 * lanes), jnp.bfloat16),
                jax.ShapeDtypeStruct((particle_count, lanes), jnp.int32),
                jax.ShapeDtypeStruct((rotations, lanes), jnp.int32),
            ),
            in_specs=[smem] * 2 + [vmem] * 7,
            out_specs=(vmem,) * 5,
            scratch_shapes=[pltpu.VMEM((halves * tail_rows, lanes), jnp.float32)],
            name="pack",
        )(me, core, particles, classes, ctf, sigma2[None], shell_of[None], rot_table, ctf_group[None])
        spread = pl.pallas_call(
            spread_kernel,
            out_shape=jax.ShapeDtypeStruct((rotations * particle_count, 2 * lanes), jnp.bfloat16),
            in_specs=[vmem, vmem],
            out_specs=vmem,
            name="spread",
        )(own_table, sources)
        swap = [(i, halves - 1 - i) for i in range(halves)]
        pieces, twins = [block[None]], [twin[None]]
        reaches = [2 ** i for i in range(1, shards.bit_length() - 1)] + [1]
        for reach in reaches if shards > 1 else ():
            held = pieces[0] if len(pieces) == 1 else jnp.concatenate(pieces, axis=0)
            pieces.append(lax.ppermute(held, "shell", [(i, i ^ reach) for i in range(shards)]))
            if len(pieces) == 3:
                pieces[-1], spread = lax.optimization_barrier((pieces[-1], spread))
            twins.append(lax.ppermute(pieces[-1], "batch", swap))
        sizes = tuple(piece.shape[0] for piece in pieces)
        blocks = sum(sizes)
        step = 8
        while step > 1 and (rotations % step or step * particle_count * blocks * lanes > 8 * 2 ** 20):
            step //= 2
        total = blocks * lanes
        part, log_rows = pl.pallas_call(
            lambda *refs: main_kernel(sizes, counts, step, *refs),
            out_shape=(
                jax.ShapeDtypeStruct((class_count, 2 * lanes), jnp.float32),
                jax.ShapeDtypeStruct((1, particle_count), jnp.float32),
            ),
            in_specs=[smem] * 2 + [vmem, pl.BlockSpec(memory_space=pl.ANY)] + [vmem] * (2 * len(pieces)),
            out_specs=(vmem, vmem),
            scratch_shapes=[
                pltpu.VMEM((class_count, total), jnp.bfloat16),
                pltpu.VMEM((halves * tail_rows, lanes), jnp.float32),
                pltpu.VMEM((blocks, group_count, lanes), jnp.float32),
                pltpu.VMEM((blocks, particle_count, lanes), jnp.float32),
                pltpu.VMEM((blocks, rotations, lanes), jnp.int32),
                pltpu.VMEM((step * particle_count, total), jnp.bfloat16),
                pltpu.VMEM((rotations * group_count, lanes), jnp.float32),
                pltpu.VMEM((rotations * group_count, class_count), jnp.float32),
                pltpu.VMEM((rotations * particle_count, class_count), jnp.float32),
                pltpu.VMEM((step * particle_count, class_count), jnp.bfloat16),
                pltpu.VMEM((rotations * particle_count, 2 * lanes), jnp.bfloat16),
                pltpu.SemaphoreType.DMA,
            ],
            name="score",
        )(me, core, group_index, spread, *pieces, *twins)
        other = lax.ppermute(part, "batch", swap)
        class_sums, class_weights = pl.pallas_call(
            add_kernel,
            out_shape=(
                jax.ShapeDtypeStruct((class_count, lanes), jnp.float32),
                jax.ShapeDtypeStruct((width, class_count), jnp.float32),
            ),
            in_specs=[vmem, vmem],
            out_specs=(vmem, vmem),
            name="add",
        )(part, other)
        return class_sums, class_weights.T, log_rows[0]

    return body


def solution(mesh):
    in_specs = (
        P(("groups", "batch"), "shell"),
        P("groups", "shell"),
        P("groups", "shell"),
        P("groups"),
        P("shell"),
        P(None, "shell"),
        P(("groups", "batch")),
    )
    out_specs = (P("groups", "shell"), P("groups", "shell"), P(("groups", "batch")))
    return jax.shard_map(build(mesh), mesh=mesh, in_specs=in_specs, out_specs=out_specs, check_vma=False)
```
